64 devices in a mesh: dp: 4 (over x, y), ep: 16 (over z, core).
Axes of the slice: x: 2, y: 2, z: 8, core: 2. Of those that a mesh axis runs over, the one named last changes fastest.
The devices are a block of a 4x4x8 slice.
Arguments:
- x_in: bfloat16 [49152, 512], P(('dp', 'ep')), parts along dimension 0
- grad_y: bfloat16 [49152, 512], P(('dp', 'ep')), parts along dimension 0
- ids_a: int32 [49152, 6], P(('dp', 'ep')), parts along dimension 0
- gate_a: float32 [49152, 6], P(('dp', 'ep')), parts along dimension 0
- ids_b: int32 [49152, 6], P(('dp', 'ep')), parts along dimension 0
- gate_b: float32 [49152, 6], P(('dp', 'ep')), parts along dimension 0
- w1_a: bfloat16 [64, 512, 384], P('ep')
- w3_a: bfloat16 [64, 512, 384], P('ep')
- w2_a: bfloat16 [64, 384, 512], P('ep')
- w1_b: bfloat16 [64, 512, 384], P('ep')
- w3_b: bfloat16 [64, 512, 384], P('ep')
- w2_b: bfloat16 [64, 384, 512], P('ep')
- wg_mid: bfloat16 [512, 2752], replicated
- wu_mid: bfloat16 [512, 2752], replicated
- wd_mid: bfloat16 [2752, 512], replicated
- wg_top: bfloat16 [512, 2752], replicated
- wu_top: bfloat16 [512, 2752], replicated
- wd_top: bfloat16 [2752, 512], replicated
Outputs:
- output 1: bfloat16 [49152, 512], P(('dp', 'ep')), parts along dimension 0
- output 2: bfloat16 [49152, 512], P(('dp', 'ep')), parts along dimension 0
- output 3: float32 [256, 512, 384], P(('dp', 'ep')), parts along dimension 0
- output 4: float32 [256, 512, 384], P(('dp', 'ep')), parts along dimension 0
- output 5: float32 [256, 384, 512], P(('dp', 'ep')), parts along dimension 0
- output 6: float32 [256, 512, 384], P(('dp', 'ep')), parts along dimension 0
- output 7: float32 [256, 512, 384], P(('dp', 'ep')), parts along dimension 0
- output 8: float32 [256, 384, 512], P(('dp', 'ep')), parts along dimension 0
- output 9: float32 [49152, 6], P(('dp', 'ep')), parts along dimension 0
- output 10: float32 [49152, 6], P(('dp', 'ep')), parts along dimension 0
There are 4 independent parts. The reference program is written for one: setup_inputs(seed, part) draws one part's arguments, and reference() takes and returns one part's arrays. A program takes and returns all parts, laid end to end along the dimension named above; an argument that names none is the same for every part.
All inputs are finite; a program needn't handle non-finite values.
Results may differ from the reference program's by a relative error of at most 0.02.
Values are sent between devices in bfloat16 or wider.
A program may use at most 768 MiB of HBM per device.

```python
import jax
import jax.numpy as jnp
from jax import lax

HIDDEN = 512
EXPERT_FF = 384
EXPERTS = 64
TOP_K = 6
DENSE_FF = 2752
TOKENS = 768
GROUP_SIZE = 16
CAPACITY = 2 * TOKENS * TOP_K // EXPERTS
PART_ROWS = GROUP_SIZE * TOKENS


def draw_routing(key):
    half_load = TOKENS * TOP_K // EXPERTS

    def one_device(dev_key):
        key_order, key_spread, key_rows = jax.random.split(dev_key, 3)
        order = jax.random.permutation(key_order, EXPERTS)
        spread = jax.random.randint(key_spread, ((EXPERTS - 4) // 2,), 0, half_load)
        paired = jnp.stack([half_load + spread, half_load - spread], axis=1).reshape(-1)
        leading = jnp.array([2 * half_load, half_load // 2, half_load // 2, half_load], jnp.int32)
        by_rank = jnp.concatenate([leading, paired.astype(jnp.int32)])
        counts = jnp.zeros((EXPERTS,), jnp.int32).at[order].set(by_rank)
        sequence = jnp.repeat(jnp.arange(EXPERTS, dtype=jnp.int32), counts, total_repeat_length=TOKENS * TOP_K)
        table = sequence.reshape(TOP_K, TOKENS).T
        return table[jax.random.permutation(key_rows, TOKENS)]

    return jax.vmap(one_device)(jax.random.split(key, GROUP_SIZE)).reshape(PART_ROWS, TOP_K)


def setup_inputs(seed: int = 0, part: int = 0) -> dict:
    keys = jax.random.split(jax.random.key(seed), 18)

    def own(index):
        return jax.random.fold_in(keys[index], part)

    def normal(key, shape, scale):
        return (jax.random.normal(key, shape, jnp.float32) * scale).astype(jnp.bfloat16)

    def gates(key):
        return jax.random.uniform(key, (PART_ROWS, TOP_K), jnp.float32, 0.5, 1.5) * TOP_K ** -0.5

    expert_in = (EXPERTS, HIDDEN, EXPERT_FF)
    expert_out = (EXPERTS, EXPERT_FF, HIDDEN)
    return {
        'x_in': normal(own(0), (PART_ROWS, HIDDEN), 1.0),
        'grad_y': normal(own(1), (PART_ROWS, HIDDEN), 1.0),
        'ids_a': draw_routing(own(2)),
        'gate_a': gates(own(3)),
        'ids_b': draw_routing(own(4)),
        'gate_b': gates(own(5)),
        'w1_a': normal(keys[6], expert_in, HIDDEN ** -0.5),
        'w3_a': normal(keys[7], expert_in, HIDDEN ** -0.5),
        'w2_a': normal(keys[8], expert_out, EXPERT_FF ** -0.5),
        'w1_b': normal(keys[9], expert_in, HIDDEN ** -0.5),
        'w3_b': normal(keys[10], expert_in, HIDDEN ** -0.5),
        'w2_b': normal(keys[11], expert_out, EXPERT_FF ** -0.5),
        'wg_mid': normal(keys[12], (HIDDEN, DENSE_FF), HIDDEN ** -0.5),
        'wu_mid': normal(keys[13], (HIDDEN, DENSE_FF), HIDDEN ** -0.5),
        'wd_mid': normal(keys[14], (DENSE_FF, HIDDEN), DENSE_FF ** -0.5),
        'wg_top': normal(keys[15], (HIDDEN, DENSE_FF), HIDDEN ** -0.5),
        'wu_top': normal(keys[16], (HIDDEN, DENSE_FF), HIDDEN ** -0.5),
        'wd_top': normal(keys[17], (DENSE_FF, HIDDEN), DENSE_FF ** -0.5),
    }


def bf16_cast(values):
    return values.astype(jnp.bfloat16).astype(jnp.float32)


def pair_rows(expert_ids):
    per_dev = expert_ids.reshape(GROUP_SIZE, TOKENS * TOP_K)
    onehot = (per_dev[:, :, None] == jnp.arange(EXPERTS, dtype=jnp.int32)).astype(jnp.int32)
    slots = jnp.sum((jnp.cumsum(onehot, axis=1) - onehot) * onehot, axis=2)
    source = jnp.arange(GROUP_SIZE, dtype=jnp.int32)[:, None]
    return ((per_dev * GROUP_SIZE + source) * CAPACITY + slots).reshape(-1)


def moe_layer(x_rows, gate, rows_of_pairs, w_one, w_three, w_two):
    repeated = jnp.broadcast_to(x_rows[:, None, :], (PART_ROWS, TOP_K, HIDDEN)).reshape(-1, HIDDEN)
    staged = jnp.zeros((EXPERTS * GROUP_SIZE * CAPACITY, HIDDEN), jnp.float32).at[rows_of_pairs].set(repeated)

    def one_expert(operands):
        tokens, mat_one, mat_three, mat_two = operands
        pre_gate = jnp.dot(tokens, mat_one, preferred_element_type=jnp.float32)
        pre_up = jnp.dot(tokens, mat_three, preferred_element_type=jnp.float32)
        hidden = bf16_cast(jax.nn.silu(pre_gate) * pre_up)
        return bf16_cast(jnp.dot(hidden, mat_two, preferred_element_type=jnp.float32))

    outputs = lax.map(one_expert, (staged.reshape(EXPERTS, GROUP_SIZE * CAPACITY, HIDDEN), w_one, w_three, w_two))
    pairs = outputs.reshape(-1, HIDDEN)[rows_of_pairs].reshape(PART_ROWS, TOP_K, HIDDEN)
    return bf16_cast(x_rows + jnp.sum(gate[:, :, None] * pairs, axis=1))


def dense_block(x_rows, w_gate, w_up, w_down):
    def one_device(rows):
        pre_gate = jnp.dot(rows, w_gate, preferred_element_type=jnp.float32)
        pre_up = jnp.dot(rows, w_up, preferred_element_type=jnp.float32)
        hidden = bf16_cast(jax.nn.silu(pre_gate) * pre_up)
        return bf16_cast(rows + jnp.dot(hidden, w_down, preferred_element_type=jnp.float32))

    return lax.map(one_device, x_rows.reshape(GROUP_SIZE, TOKENS, HIDDEN)).reshape(PART_ROWS, HIDDEN)


def reference(x_in, grad_y, ids_a, gate_a, ids_b, gate_b, w1_a, w3_a, w2_a, w1_b, w3_b, w2_b, wg_mid, wu_mid, wd_mid, wg_top, wu_top, wd_top):
    rows_a = pair_rows(ids_a)
    rows_b = pair_rows(ids_b)
    dense_mid = (wg_mid.astype(jnp.float32), wu_mid.astype(jnp.float32), wd_mid.astype(jnp.float32))
    dense_top = (wg_top.astype(jnp.float32), wu_top.astype(jnp.float32), wd_top.astype(jnp.float32))

    def forward(x_start, mix_a, mix_b, one_a, three_a, two_a, one_b, three_b, two_b):
        x_a = moe_layer(x_start, mix_a, rows_a, one_a, three_a, two_a)
        x_mid = dense_block(x_a, dense_mid[0], dense_mid[1], dense_mid[2])
        x_b = moe_layer(x_mid, mix_b, rows_b, one_b, three_b, two_b)
        return dense_block(x_b, dense_top[0], dense_top[1], dense_top[2])

    y_out, pullback = jax.vjp(forward, x_in.astype(jnp.float32), gate_a, gate_b,
                              w1_a.astype(jnp.float32), w3_a.astype(jnp.float32), w2_a.astype(jnp.float32),
                              w1_b.astype(jnp.float32), w3_b.astype(jnp.float32), w2_b.astype(jnp.float32))
    grads = pullback(grad_y.astype(jnp.float32))
    return (y_out.astype(jnp.bfloat16), grads[0].astype(jnp.bfloat16), grads[3], grads[4], grads[5],
            grads[6], grads[7], grads[8], grads[1], grads[2])
```

```python
import functools

import jax
import jax.numpy as jnp
from jax import lax
from jax.experimental import pallas as pl
from jax.experimental.pallas import tpu as pltpu
from jax.sharding import PartitionSpec as P

CONTRACT_LAST = (((1,), (1,)), ((), ()))
CONTRACT_FIRST = (((0,), (0,)), ((), ()))
F32 = jnp.float32
BF16 = jnp.bfloat16


def dot(a, b, dims=(((1,), (0,)), ((), ()))):
    return lax.dot_general(a, b, dims, preferred_element_type=F32)


def swiglu_grad(pre_gate, pre_up, grad_hidden):
    sigma = jax.nn.sigmoid(pre_gate)
    grad_gate = grad_hidden * pre_up * sigma * (1.0 + pre_gate * (1.0 - sigma))
    grad_up = grad_hidden * pre_gate * sigma
    return grad_gate.astype(BF16), grad_up.astype(BF16)


def dense_forward(x_rows, w_gate, w_up, w_down):
    pre_gate = dot(x_rows, w_gate)
    pre_up = dot(x_rows, w_up)
    hidden = (jax.nn.silu(pre_gate) * pre_up).astype(BF16)
    branch = dot(hidden, w_down)
    return (x_rows.astype(F32) + branch).astype(BF16)


def dense_backward(x_rows, grad_out, w_gate, w_up, w_down):
    pre_gate = dot(x_rows, w_gate)
    pre_up = dot(x_rows, w_up)
    grad_hidden = dot(grad_out, w_down, CONTRACT_LAST)
    grad_gate, grad_up = swiglu_grad(pre_gate, pre_up, grad_hidden)
    branch = dot(grad_gate, w_gate, CONTRACT_LAST) + dot(grad_up, w_up, CONTRACT_LAST)
    return (grad_out.astype(F32) + branch).astype(BF16)


def pick_rows(meta, expert, capacity):
    n_tok = meta.shape[1]
    slots = lax.broadcasted_iota(jnp.int32, (capacity, n_tok), 0).astype(F32)
    return meta[expert:expert + 1, :] == slots


def place_rows(meta_t, expert, capacity):
    n_tok = meta_t.shape[0]
    slots = lax.broadcasted_iota(jnp.int32, (n_tok, capacity), 1).astype(F32)
    return jnp.where(meta_t[:, expert:expert + 1] == slots, 1.0, 0.0).astype(BF16)


def pack(meta, n_local, capacity):
    masks = [jnp.where(pick_rows(meta, e, capacity), 1.0, 0.0).astype(BF16) for e in range(n_local)]
    return jnp.concatenate(masks, axis=0)


def forward_kernel(n_local, capacity, meta_ref, meta_t_ref, x_ref, w1_ref, w3_ref, w2_ref, out_ref, tok, res):
    pair = x_ref.shape[0]
    for i in range(pair):
        tok[i] = dot(pack(meta_ref[i], n_local, capacity), x_ref[i]).astype(BF16)
    for e in range(n_local):
        rows = slice(e * capacity, (e + 1) * capacity)
        a = jnp.concatenate([tok[i, rows] for i in range(pair)], axis=0)
        hidden = (jax.nn.silu(dot(a, w1_ref[e])) * dot(a, w3_ref[e])).astype(BF16)
        o = dot(hidden, w2_ref[e]).astype(BF16)
        for i in range(pair):
            res[i, rows] = o[i * capacity:(i + 1) * capacity]
    for i in range(pair):
        for e in range(n_local):
            part = dot(place_rows(meta_t_ref[i], e, capacity), res[i, e * capacity:(e + 1) * capacity])
            part = meta_t_ref[i, :, n_local + e:n_local + e + 1] * part
            out_ref[i] = part if e == 0 else out_ref[i] + part


def backward_kernel(n_local, capacity, meta_ref, meta_t_ref, x_ref, c_ref, w1_ref, w3_ref, w2_ref,
                    out_ref, mix_ref, dw1_ref, dw3_ref, dw2_ref, tok, cot, res):
    pair = x_ref.shape[0]

    @pl.when(pl.program_id(0) == 0)
    def _():
        dw1_ref[...] = jnp.zeros_like(dw1_ref)
        dw3_ref[...] = jnp.zeros_like(dw3_ref)
        dw2_ref[...] = jnp.zeros_like(dw2_ref)

    for i in range(pair):
        picked = pack(meta_ref[i], n_local, capacity)
        tok[i] = dot(picked, x_ref[i]).astype(BF16)
        cot[i] = dot(picked, c_ref[i]).astype(BF16)
    for e in range(n_local):
        rows = slice(e * capacity, (e + 1) * capacity)
        a = jnp.concatenate([tok[i, rows] for i in range(pair)], axis=0)
        c = jnp.concatenate([cot[i, rows] for i in range(pair)], axis=0)
        gate = jnp.concatenate(
            [jnp.sum(jnp.where(pick_rows(meta_ref[i], e, capacity), meta_ref[i, n_local + e:n_local + e + 1, :], 0.0),
                     axis=1, keepdims=True) for i in range(pair)], axis=0)
        pre_gate = dot(a, w1_ref[e])
        pre_up = dot(a, w3_ref[e])
        hidden = (jax.nn.silu(pre_gate) * pre_up).astype(BF16)
        o = dot(hidden, w2_ref[e]).astype(BF16)
        cf = c.astype(F32)
        mix = jnp.sum(cf * o.astype(F32), axis=1, keepdims=True)
        for i in range(pair):
            own = mix[i * capacity:(i + 1) * capacity]
            mix_ref[i, e:e + 1, :] = jnp.sum(jnp.where(pick_rows(meta_ref[i], e, capacity), own, 0.0), axis=0, keepdims=True)
        grad_o = (gate * cf).astype(BF16)
        dw2_ref[e] += dot(hidden, grad_o, CONTRACT_FIRST)
        grad_hidden = dot(grad_o, w2_ref[e], CONTRACT_LAST)
        grad_gate, grad_up = swiglu_grad(pre_gate, pre_up, grad_hidden)
        dw1_ref[e] += dot(a, grad_gate, CONTRACT_FIRST)
        dw3_ref[e] += dot(a, grad_up, CONTRACT_FIRST)
        du = (dot(grad_gate, w1_ref[e], CONTRACT_LAST) + dot(grad_up, w3_ref[e], CONTRACT_LAST)).astype(BF16)
        for i in range(pair):
            res[i, rows] = du[i * capacity:(i + 1) * capacity]
    for i in range(pair):
        placed = jnp.concatenate([place_rows(meta_t_ref[i], e, capacity) for e in range(n_local)], axis=1)
        out_ref[i] = dot(placed, res[i])


def whole(shape):
    return pl.BlockSpec(shape, lambda g: (0,) * len(shape))


def chunk(shape):
    return pl.BlockSpec(shape, lambda g: (g,) + (0,) * (len(shape) - 1))


PAIR = 2


def expert_forward(meta, meta_t, x_all, w1, w3, w2, capacity):
    group, n_tok, width = x_all.shape
    n_local, _, ff = w1.shape
    packed = n_local * capacity
    return pl.pallas_call(
        functools.partial(forward_kernel, n_local, capacity),
        grid=(group // PAIR,),
        in_specs=[chunk((PAIR,) + meta.shape[1:]), chunk((PAIR,) + meta_t.shape[1:]), chunk((PAIR, n_tok, width)),
                  whole(w1.shape), whole(w3.shape), whole(w2.shape)],
        out_specs=chunk((PAIR, n_tok, width)),
        out_shape=jax.ShapeDtypeStruct((group, n_tok, width), F32),
        scratch_shapes=[pltpu.VMEM((PAIR, packed, width), BF16)] * 2,
        compiler_params=pltpu.CompilerParams(vmem_limit_bytes=60 * 1024 * 1024),
        cost_estimate=pl.CostEstimate(flops=40 * 10**9, bytes_accessed=40 * 10**6, transcendentals=0),
        name="expert_forward",
    )(meta, meta_t, x_all, w1, w3, w2)


def expert_backward(meta, meta_t, x_all, c_all, w1, w3, w2, capacity):
    group, n_tok, width = x_all.shape
    n_local, _, ff = w1.shape
    packed = n_local * capacity
    return pl.pallas_call(
        functools.partial(backward_kernel, n_local, capacity),
        grid=(group // PAIR,),
        in_specs=[chunk((PAIR,) + meta.shape[1:]), chunk((PAIR,) + meta_t.shape[1:]),
                  chunk((PAIR, n_tok, width)), chunk((PAIR, n_tok, width)),
                  whole(w1.shape), whole(w3.shape), whole(w2.shape)],
        out_specs=[chunk((PAIR, n_tok, width)), chunk((PAIR, n_local, n_tok)),
                   whole(w1.shape), whole(w3.shape), whole(w2.shape)],
        out_shape=[jax.ShapeDtypeStruct((group, n_tok, width), F32), jax.ShapeDtypeStruct((group, n_local, n_tok), F32),
                   jax.ShapeDtypeStruct(w1.shape, F32), jax.ShapeDtypeStruct(w3.shape, F32),
                   jax.ShapeDtypeStruct(w2.shape, F32)],
        scratch_shapes=[pltpu.VMEM((PAIR, packed, width), BF16)] * 3,
        compiler_params=pltpu.CompilerParams(vmem_limit_bytes=60 * 1024 * 1024),
        cost_estimate=pl.CostEstimate(flops=80 * 10**9, bytes_accessed=60 * 10**6, transcendentals=0),
        name="expert_backward",
    )(meta, meta_t, x_all, c_all, w1, w3, w2)


def solution(mesh):
    group = mesh.shape['ep']
    tok_spec = P(('dp', 'ep'), None)
    exp_spec = P('ep', None, None)
    full_spec = P(None, None)
    grad_spec = P(('dp', 'ep'), None, None)

    def device_program(x_in, grad_y, ids_a, gate_a, ids_b, gate_b, w1_a, w3_a, w2_a, w1_b, w3_b, w2_b,
                       wg_mid, wu_mid, wd_mid, wg_top, wu_top, wd_top):
        n_tok, width = x_in.shape
        top_k = ids_a.shape[1]
        n_local = w1_a.shape[0]
        n_exp = n_local * group
        capacity = 2 * n_tok * top_k // n_exp
        me = lax.axis_index('ep')

        heads = jnp.concatenate([ids_a.astype(F32), gate_a, ids_b.astype(F32), gate_b], axis=1).T
        heads = lax.all_gather(heads, 'ep', axis=0, tiled=False)
        mine = (me * n_local + jnp.arange(n_local, dtype=jnp.int32)).astype(F32)
        earlier = jnp.triu(jnp.ones((n_tok, n_tok), BF16), 1)

        def route(ids, gate):
            match = ids[:, None, :, :] == mine[None, :, None, None]
            chosen = jnp.any(match, axis=2)
            gates = jnp.sum(jnp.where(match, gate[:, None, :, :], 0.0), axis=2)
            before = dot(chosen.astype(BF16).reshape(group * n_local, n_tok), earlier).reshape(chosen.shape)
            meta = jnp.concatenate([jnp.where(chosen, before, -1.0), gates], axis=1)
            return meta, jnp.swapaxes(meta, 1, 2)

        meta_a, meta_at = route(heads[:, :top_k], heads[:, top_k:2 * top_k])
        meta_b, meta_bt = route(heads[:, 2 * top_k:3 * top_k], heads[:, 3 * top_k:])

        def gather(rows):
            return lax.all_gather(rows, 'ep', axis=0, tiled=False)

        def scatter_sum(parts):
            return lax.psum_scatter(parts.reshape(group * n_tok, width), 'ep', scatter_dimension=0, tiled=True)

        def add_rows(rows, total):
            return (rows.astype(F32) + total).astype(BF16)

        def return_mix(mix, ids):
            home = lax.all_to_all(mix, 'ep', 0, 0, tiled=True).reshape(n_exp, n_tok)
            picked = ids.T[:, None, :] == jnp.arange(n_exp, dtype=jnp.int32)[None, :, None]
            return jnp.sum(jnp.where(picked, home[None], 0.0), axis=1).T

        x_a = add_rows(x_in, scatter_sum(expert_forward(meta_a, meta_at, gather(x_in), w1_a, w3_a, w2_a, capacity)))
        x_mid = dense_forward(x_a, wg_mid, wu_mid, wd_mid)
        held_b = gather(x_mid)
        x_b = add_rows(x_mid, scatter_sum(expert_forward(meta_b, meta_bt, held_b, w1_b, w3_b, w2_b, capacity)))
        y_out = dense_forward(x_b, wg_top, wu_top, wd_top)

        x_b, grad_y, y_out = lax.optimization_barrier((x_b, grad_y, y_out))
        grad_b = dense_backward(x_b, grad_y, wg_top, wu_top, wd_top)
        part_b, mix_b, dw1_b, dw3_b, dw2_b = expert_backward(
            meta_b, meta_bt, held_b, gather(grad_b), w1_b, w3_b, w2_b, capacity)
        x_again, grad_b2 = lax.optimization_barrier((x_in, grad_b))
        held_a = gather(x_again)
        grad_mid = add_rows(grad_b2, scatter_sum(part_b))
        grad_a = dense_backward(x_a, grad_mid, wg_mid, wu_mid, wd_mid)
        part_a, mix_a, dw1_a, dw3_a, dw2_a = expert_backward(
            meta_a, meta_at, held_a, gather(grad_a), w1_a, w3_a, w2_a, capacity)
        dx_in = add_rows(grad_a, scatter_sum(part_a))
        return (y_out, dx_in, dw1_a, dw3_a, dw2_a, dw1_b, dw3_b, dw2_b,
                return_mix(mix_a, ids_a), return_mix(mix_b, ids_b))

    in_specs = (tok_spec, tok_spec, tok_spec, tok_spec, tok_spec, tok_spec,
                exp_spec, exp_spec, exp_spec, exp_spec, exp_spec, exp_spec,
                full_spec, full_spec, full_spec, full_spec, full_spec, full_spec)
    out_specs = (tok_spec, tok_spec, grad_spec, grad_spec, grad_spec, grad_spec, grad_spec, grad_spec, tok_spec, tok_spec)
    return jax.shard_map(device_program, mesh=mesh, in_specs=in_specs, out_specs=out_specs, check_vma=False)
```

```python
import functools

import jax
import jax.numpy as jnp
from jax import lax
from jax.experimental import pallas as pl
from jax.experimental.pallas import tpu as pltpu
from jax.sharding import PartitionSpec as P

CONTRACT_LAST = (((1,), (1,)), ((), ()))
CONTRACT_FIRST = (((0,), (0,)), ((), ()))
F32 = jnp.float32
BF16 = jnp.bfloat16


def dot(a, b, dims=(((1,), (0,)), ((), ()))):
    return lax.dot_general(a, b, dims, preferred_element_type=F32)


def swiglu_grad(pre_gate, pre_up, grad_hidden):
    sigma = jax.nn.sigmoid(pre_gate)
    grad_gate = grad_hidden * pre_up * sigma * (1.0 + pre_gate * (1.0 - sigma))
    grad_up = grad_hidden * pre_gate * sigma
    return grad_gate.astype(BF16), grad_up.astype(BF16)


def dense_forward(x_rows, w_gate, w_up, w_down):
    pre_gate = dot(x_rows, w_gate)
    pre_up = dot(x_rows, w_up)
    hidden = (jax.nn.silu(pre_gate) * pre_up).astype(BF16)
    branch = dot(hidden, w_down)
    return (x_rows.astype(F32) + branch).astype(BF16)


def dense_backward(x_rows, grad_out, w_gate, w_up, w_down):
    pre_gate = dot(x_rows, w_gate)
    pre_up = dot(x_rows, w_up)
    grad_hidden = dot(grad_out, w_down, CONTRACT_LAST)
    grad_gate, grad_up = swiglu_grad(pre_gate, pre_up, grad_hidden)
    branch = dot(grad_gate, w_gate, CONTRACT_LAST) + dot(grad_up, w_up, CONTRACT_LAST)
    return (grad_out.astype(F32) + branch).astype(BF16)


def pick_rows(meta, expert, capacity):
    n_tok = meta.shape[1]
    slots = lax.broadcasted_iota(jnp.int32, (capacity, n_tok), 0).astype(F32)
    return meta[expert:expert + 1, :] == slots


def place_rows(meta_t, expert, capacity):
    n_tok = meta_t.shape[0]
    slots = lax.broadcasted_iota(jnp.int32, (n_tok, capacity), 1).astype(F32)
    return jnp.where(meta_t[:, expert:expert + 1] == slots, 1.0, 0.0).astype(BF16)


def pack(meta, n_local, capacity):
    masks = [jnp.where(pick_rows(meta, e, capacity), 1.0, 0.0).astype(BF16) for e in range(n_local)]
    return jnp.concatenate(masks, axis=0)


def forward_kernel(n_local, capacity, meta_ref, meta_t_ref, x_ref, w1_ref, w3_ref, w2_ref, out_ref, tok, res):
    pair = x_ref.shape[0]
    for i in range(pair):
        tok[i] = dot(pack(meta_ref[i], n_local, capacity), x_ref[i]).astype(BF16)
    for e in range(n_local):
        rows = slice(e * capacity, (e + 1) * capacity)
        a = jnp.concatenate([tok[i, rows] for i in range(pair)], axis=0)
        hidden = (jax.nn.silu(dot(a, w1_ref[e])) * dot(a, w3_ref[e])).astype(BF16)
        o = dot(hidden, w2_ref[e]).astype(BF16)
        for i in range(pair):
            res[i, rows] = o[i * capacity:(i + 1) * capacity]
    for i in range(pair):
        for e in range(n_local):
            part = dot(place_rows(meta_t_ref[i], e, capacity), res[i, e * capacity:(e + 1) * capacity])
            part = meta_t_ref[i, :, n_local + e:n_local + e + 1] * part
            out_ref[i] = part if e == 0 else out_ref[i] + part


def recompute_kernel(n_local, capacity, meta_ref, *refs):
    *x_refs, w1_ref, w3_ref, w2_ref, tok_ref, gate_ref, up_ref, hid_ref, o_ref = refs
    pair = meta_ref.shape[0]
    for i in range(pair):
        x = jnp.concatenate([x_ref[i] for x_ref in x_refs], axis=0)
        tok_ref[i] = dot(pack(meta_ref[i], n_local, capacity), x).astype(BF16)
    for e in range(n_local):
        rows = slice(e * capacity, (e + 1) * capacity)
        a = jnp.concatenate([tok_ref[i, rows] for i in range(pair)], axis=0)
        pre_gate = dot(a, w1_ref[e])
        pre_up = dot(a, w3_ref[e])
        hidden = (jax.nn.silu(pre_gate) * pre_up).astype(BF16)
        o = dot(hidden, w2_ref[e]).astype(BF16)
        for i in range(pair):
            own = slice(i * capacity, (i + 1) * capacity)
            gate_ref[i, rows] = pre_gate[own]
            up_ref[i, rows] = pre_up[own]
            hid_ref[i, rows] = hidden[own]
            o_ref[i, rows] = o[own]


def cotangent_kernel(n_local, capacity, meta_ref, meta_t_ref, c_ref, gate_ref, up_ref, o_ref, w1_ref, w3_ref, w2_ref,
                     out_ref, mix_ref, go_ref, gg_ref, gu_ref, cot, res):
    pair = c_ref.shape[0]
    for i in range(pair):
        cot[i] = dot(pack(meta_ref[i], n_local, capacity), c_ref[i]).astype(BF16)
    for e in range(n_local):
        rows = slice(e * capacity, (e + 1) * capacity)

        def both(ref):
            return jnp.concatenate([ref[i, rows] for i in range(pair)], axis=0)

        cf = both(cot).astype(F32)
        gate = jnp.concatenate(
            [jnp.sum(jnp.where(pick_rows(meta_ref[i], e, capacity), meta_ref[i, n_local + e:n_local + e + 1, :], 0.0),
                     axis=1, keepdims=True) for i in range(pair)], axis=0)
        mix = jnp.sum(cf * both(o_ref).astype(F32), axis=1, keepdims=True)
        for i in range(pair):
            own = mix[i * capacity:(i + 1) * capacity]
            mix_ref[i, e:e + 1, :] = jnp.sum(jnp.where(pick_rows(meta_ref[i], e, capacity), own, 0.0), axis=0, keepdims=True)
        grad_o = (gate * cf).astype(BF16)
        grad_hidden = dot(grad_o, w2_ref[e], CONTRACT_LAST)
        grad_gate, grad_up = swiglu_grad(both(gate_ref), both(up_ref), grad_hidden)
        du = (dot(grad_gate, w1_ref[e], CONTRACT_LAST) + dot(grad_up, w3_ref[e], CONTRACT_LAST)).astype(BF16)
        for i in range(pair):
            own = slice(i * capacity, (i + 1) * capacity)
            res[i, rows] = du[own]
            go_ref[i, rows] = grad_o[own]
            gg_ref[i, rows] = grad_gate[own]
            gu_ref[i, rows] = grad_up[own]
    for i in range(pair):
        placed = jnp.concatenate([place_rows(meta_t_ref[i], e, capacity) for e in range(n_local)], axis=1)
        out_ref[i] = dot(placed, res[i])


def weight_kernel(n_local, capacity, tok_ref, hid_ref, go_ref, gg_ref, gu_ref, dw1_ref, dw3_ref, dw2_ref):
    pair = tok_ref.shape[0]

    @pl.when(pl.program_id(0) == 0)
    def _():
        dw1_ref[...] = jnp.zeros_like(dw1_ref)
        dw3_ref[...] = jnp.zeros_like(dw3_ref)
        dw2_ref[...] = jnp.zeros_like(dw2_ref)

    for e in range(n_local):
        rows = slice(e * capacity, (e + 1) * capacity)

        def both(ref):
            return jnp.concatenate([ref[i, rows] for i in range(pair)], axis=0)

        a = both(tok_ref)
        dw2_ref[e] += dot(both(hid_ref), both(go_ref), CONTRACT_FIRST)
        dw1_ref[e] += dot(a, both(gg_ref), CONTRACT_FIRST)
        dw3_ref[e] += dot(a, both(gu_ref), CONTRACT_FIRST)


def whole(shape):
    return pl.BlockSpec(shape, lambda g: (0,) * len(shape))


def chunk(shape):
    return pl.BlockSpec(shape, lambda g: (g,) + (0,) * (len(shape) - 1))


PAIR = 2


def expert_forward(meta, meta_t, x_all, w1, w3, w2, capacity):
    group, n_tok, width = x_all.shape
    n_local, _, ff = w1.shape
    packed = n_local * capacity
    return pl.pallas_call(
        functools.partial(forward_kernel, n_local, capacity),
        grid=(group // PAIR,),
        in_specs=[chunk((PAIR,) + meta.shape[1:]), chunk((PAIR,) + meta_t.shape[1:]), chunk((PAIR, n_tok, width)),
                  whole(w1.shape), whole(w3.shape), whole(w2.shape)],
        out_specs=chunk((PAIR, n_tok, width)),
        out_shape=jax.ShapeDtypeStruct((group, n_tok, width), F32),
        scratch_shapes=[pltpu.VMEM((PAIR, packed, width), BF16)] * 2,
        compiler_params=pltpu.CompilerParams(vmem_limit_bytes=60 * 1024 * 1024),
        cost_estimate=pl.CostEstimate(flops=40 * 10**9, bytes_accessed=40 * 10**6, transcendentals=0),
        name="expert_forward",
    )(meta, meta_t, x_all, w1, w3, w2)


def call(kernel, name, ins, outs, scratch, flops):
    group = ins[0].shape[0]

    def spec(array):
        return chunk((PAIR,) + array.shape[1:]) if array.shape[0] == group else whole(array.shape)

    return pl.pallas_call(
        kernel,
        grid=(group // PAIR,),
        in_specs=[spec(array) for array in ins],
        out_specs=[spec(array) for array in outs],
        out_shape=outs,
        scratch_shapes=scratch,
        compiler_params=pltpu.CompilerParams(vmem_limit_bytes=60 * 1024 * 1024),
        cost_estimate=pl.CostEstimate(flops=flops, bytes_accessed=60 * 10**6, transcendentals=0),
        name=name,
    )(*ins)


def expert_recompute(meta, pieces, w1, w3, w2, capacity):
    group, _, width = pieces[0].shape
    n_local, _, ff = w1.shape
    packed = n_local * capacity
    outs = [jax.ShapeDtypeStruct((group, packed, size), dtype)
            for size, dtype in ((width, BF16), (ff, F32), (ff, F32), (ff, BF16), (width, BF16))]
    return call(functools.partial(recompute_kernel, n_local, capacity), "expert_recompute",
                (meta, *pieces, w1, w3, w2), outs, [], 30 * 10**9)


def expert_cotangent(meta, meta_t, c_all, pre_gate, pre_up, o, w1, w3, w2, capacity):
    group, n_tok, width = c_all.shape
    n_local, _, ff = w1.shape
    packed = n_local * capacity
    outs = [jax.ShapeDtypeStruct((group, n_tok, width), F32), jax.ShapeDtypeStruct((group, n_local, n_tok), F32),
            jax.ShapeDtypeStruct((group, packed, width), BF16), jax.ShapeDtypeStruct((group, packed, ff), BF16),
            jax.ShapeDtypeStruct((group, packed, ff), BF16)]
    return call(functools.partial(cotangent_kernel, n_local, capacity), "expert_cotangent",
                (meta, meta_t, c_all, pre_gate, pre_up, o, w1, w3, w2), outs,
                [pltpu.VMEM((PAIR, packed, width), BF16)] * 2, 40 * 10**9)


def expert_weights(tok, hidden, grad_o, grad_gate, grad_up, n_local, capacity):
    width, ff = tok.shape[2], hidden.shape[2]
    outs = [jax.ShapeDtypeStruct((n_local, width, ff), F32), jax.ShapeDtypeStruct((n_local, width, ff), F32),
            jax.ShapeDtypeStruct((n_local, ff, width), F32)]
    return call(functools.partial(weight_kernel, n_local, capacity), "expert_weights",
                (tok, hidden, grad_o, grad_gate, grad_up), outs, [], 20 * 10**9)


def solution(mesh):
    group = mesh.shape['ep']
    tok_spec = P(('dp', 'ep'), None)
    exp_spec = P('ep', None, None)
    full_spec = P(None, None)
    grad_spec = P(('dp', 'ep'), None, None)

    def device_program(x_in, grad_y, ids_a, gate_a, ids_b, gate_b, w1_a, w3_a, w2_a, w1_b, w3_b, w2_b,
                       wg_mid, wu_mid, wd_mid, wg_top, wu_top, wd_top):
        n_tok, width = x_in.shape
        top_k = ids_a.shape[1]
        n_local = w1_a.shape[0]
        n_exp = n_local * group
        capacity = 2 * n_tok * top_k // n_exp
        me = lax.axis_index('ep')

        def share(ids, gate):
            return lax.all_gather(jnp.concatenate([ids.astype(F32), gate], axis=1).T, 'ep', axis=0, tiled=False)

        mine = (me * n_local + jnp.arange(n_local, dtype=jnp.int32)).astype(F32)
        earlier = jnp.triu(jnp.ones((n_tok, n_tok), BF16), 1)

        def route(heads):
            ids, gate = heads[:, :top_k], heads[:, top_k:]
            match = ids[:, None, :, :] == mine[None, :, None, None]
            chosen = jnp.any(match, axis=2)
            gates = jnp.sum(jnp.where(match, gate[:, None, :, :], 0.0), axis=2)
            before = dot(chosen.astype(BF16).reshape(group * n_local, n_tok), earlier).reshape(chosen.shape)
            meta = jnp.concatenate([jnp.where(chosen, before, -1.0), gates], axis=1)
            return meta, jnp.swapaxes(meta, 1, 2)

        def gather(rows):
            return lax.all_gather(rows, 'ep', axis=0, tiled=False)

        def scatter_sum(parts):
            return lax.psum_scatter(parts.reshape(group * n_tok, width), 'ep', scatter_dimension=0, tiled=True)

        def add_rows(rows, total):
            return (rows.astype(F32) + total).astype(BF16)

        def return_mix(mix, ids):
            home = lax.all_to_all(mix, 'ep', 0, 0, tiled=True).reshape(n_exp, n_tok)
            picked = ids.T[:, None, :] == jnp.arange(n_exp, dtype=jnp.int32)[None, :, None]
            return jnp.sum(jnp.where(picked, home[None], 0.0), axis=1).T

        def backward(meta, meta_t, held, grad_all, w1, w3, w2):
            tok, pre_gate, pre_up, hidden, o = expert_recompute(meta, held, w1, w3, w2, capacity)
            part, mix, grad_o, grad_gate, grad_up = expert_cotangent(
                meta, meta_t, grad_all, pre_gate, pre_up, o, w1, w3, w2, capacity)
            return part, mix, (tok, hidden, grad_o, grad_gate, grad_up, n_local, capacity)

        meta_a, meta_at = route(share(ids_a, gate_a))
        held = gather(x_in)
        part = expert_forward(meta_a, meta_at, held, w1_a, w3_a, w2_a, capacity)
        ids_late, gate_late, part = lax.optimization_barrier((ids_b, gate_b, part))
        meta_b, meta_bt = route(share(ids_late, gate_late))
        x_a = add_rows(x_in, scatter_sum(part))
        x_mid = dense_forward(x_a, wg_mid, wu_mid, wd_mid)
        held_b = gather(x_mid)
        x_b = add_rows(x_mid, scatter_sum(expert_forward(meta_b, meta_bt, held_b, w1_b, w3_b, w2_b, capacity)))
        y_out = dense_forward(x_b, wg_top, wu_top, wd_top)

        cuts = (n_tok // 4, 3 * (n_tok // 4))
        x_first, x_second, x_third = x_in[:cuts[0]], x_in[cuts[0]:cuts[1]], x_in[cuts[1]:]
        x_b, grad_y, x_first = lax.optimization_barrier((x_b, grad_y, x_first))
        grad_b = dense_backward(x_b, grad_y, wg_top, wu_top, wd_top)
        grad_b, held_b, x_second, first_a = lax.optimization_barrier((grad_b, held_b, x_second, gather(x_first)))
        grads_b, y_out = lax.optimization_barrier((gather(grad_b), y_out))
        part_b, mix_b, for_weights_b = backward(meta_b, meta_bt, (held_b,), grads_b, w1_b, w3_b, w2_b)
        part_b, second_a = lax.optimization_barrier((part_b, gather(x_second)))
        total_b, dw1_b, dw3_b, dw2_b = lax.optimization_barrier((scatter_sum(part_b),) + tuple(expert_weights(*for_weights_b)))
        grad_mid, x_third = lax.optimization_barrier((add_rows(grad_b, total_b), x_third))
        grad_a = dense_backward(x_a, grad_mid, wg_mid, wu_mid, wd_mid)
        grad_a, third_a = lax.optimization_barrier((grad_a, gather(x_third)))
        part_a, mix_a, for_weights_a = backward(meta_a, meta_at, (first_a, second_a, third_a), gather(grad_a), w1_a, w3_a, w2_a)
        dx_in = add_rows(grad_a, scatter_sum(part_a))
        dw1_a, dw3_a, dw2_a = expert_weights(*for_weights_a)
        return (y_out, dx_in, dw1_a, dw3_a, dw2_a, dw1_b, dw3_b, dw2_b,
                return_mix(mix_a, ids_a), return_mix(mix_b, ids_b))

    in_specs = (tok_spec, tok_spec, tok_spec, tok_spec, tok_spec, tok_spec,
                exp_spec, exp_spec, exp_spec, exp_spec, exp_spec, exp_spec,
                full_spec, full_spec, full_spec, full_spec, full_spec, full_spec)
    out_specs = (tok_spec, tok_spec, grad_spec, grad_spec, grad_spec, grad_spec, grad_spec, grad_spec, tok_spec, tok_spec)
    return jax.shard_map(device_program, mesh=mesh, in_specs=in_specs, out_specs=out_specs, check_vma=False)
```
